256 devices in a mesh: outer: 16 (over z_lo, y), inner: 16 (over x, z_hi, core).
Axes of the slice: x: 4, y: 4, z: 8 (z_hi: 2, z_lo: 4; z = z_hi * 4 + z_lo), core: 2. Of those that a mesh axis runs over, the one named last changes fastest.
Arguments:
- stem_real: float32 [16, 16, 256, 512], P('outer', 'inner'), may hold values from -6 to 6
- stem_imag: float32 [16, 16, 256, 512], P('outer', 'inner'), may hold values from -6 to 6
- branch_real: float32 [4, 512, 512], replicated, may hold values from -0.1875 to 0.1875
- branch_imag: float32 [4, 512, 512], replicated, may hold values from -0.1875 to 0.1875
- orders: int32 [4, 512], replicated, may hold values from 0 to 511, each once within a row
Outputs:
- out_real: float32 [16, 16, 256, 512], P('outer', 'inner')
- out_imag: float32 [16, 16, 256, 512], P('outer', 'inner')
The draws below stay inside these ranges and needn't reach their ends.
Inputs may be any that keep to these rules, and one draw needn't show every extreme that they name: Each row of orders holds every index of 0 to 511 once.
All inputs are finite; a program needn't handle non-finite values.
Results may differ from the reference program's by a relative error of at most 0.0001.
Values sent between devices are 32-bit elements; how exact they have to be, the bound alone decides.
No kernel may reach another device: no remote copies, remote signals or barrier semaphores. Data moves between devices by JAX's collectives and lax.ppermute only.
A program may use at most 64 MiB of HBM per device.

```python
import jax
import jax.numpy as jnp
from jax import lax

K = 512
ROWS = 256
PRODUCTS = 4
N_OUTER = 16
N_INNER = 16


def shard_levels(own_key, shape, pieces, least, high):
    loudness = 1.0
    for position, shards_of in pieces:
        draws = jax.random.uniform(jax.random.fold_in(jax.random.fold_in(own_key, 6), position), (shards_of,), jnp.float32, least / len(pieces), high / len(pieces))
        loudness = loudness * jnp.repeat(jnp.exp(draws), shape[position] // shards_of).reshape((-1,) + (1,) * (len(shape) - 1 - position))
    return loudness


def scatter_about(own_key, extent, spread, bound, cuts=(), dtype=jnp.bfloat16):
    values = spread * jax.random.normal(own_key, extent, jnp.float32)
    if cuts:
        values = values * shard_levels(own_key, extent, cuts, -0.22, 0.18)
    return jnp.clip(values, -bound, bound).astype(dtype)


def setup_inputs(seed: int = 0) -> dict:
    arg_keys = jax.random.split(jax.random.key(seed), 6)
    return {
        "stem_real": scatter_about(arg_keys[0], (N_OUTER, N_INNER, ROWS, K), 1.0, 6.0, ((0, 16), (1, 16)), jnp.float32),
        "stem_imag": scatter_about(arg_keys[1], (N_OUTER, N_INNER, ROWS, K), 1.0, 6.0, ((0, 16), (1, 16)), jnp.float32),
        "branch_real": scatter_about(arg_keys[2], (PRODUCTS, K, K), (2 * K) ** -0.5, 0.1875, (), jnp.float32),
        "branch_imag": scatter_about(arg_keys[3], (PRODUCTS, K, K), (2 * K) ** -0.5, 0.1875, (), jnp.float32),
        "orders": jax.vmap(lambda own: jax.random.permutation(own, K))(jax.random.split(arg_keys[4], PRODUCTS)).reshape((PRODUCTS, K)).astype(jnp.int32),
    }


def multiply(plane_real, plane_imag, branch_real, branch_imag, order):
    shape = plane_real.shape
    width = shape[-1]
    left_real = plane_real[..., order].reshape(-1, width)
    left_imag = plane_imag[..., order].reshape(-1, width)
    first = jnp.dot(left_real, branch_real, precision=lax.Precision.HIGHEST, preferred_element_type=jnp.float32)
    second = jnp.dot(left_imag, branch_imag, precision=lax.Precision.HIGHEST, preferred_element_type=jnp.float32)
    third = jnp.dot(left_real + left_imag, branch_real + branch_imag, precision=lax.Precision.HIGHEST, preferred_element_type=jnp.float32)
    return (first - second).reshape(shape), (third - first - second).reshape(shape)


def swap_group(plane, groups, axis_pos):
    outer_n, inner_n, rows_n, width = plane.shape
    viewed = plane.reshape(outer_n, inner_n, rows_n, groups, width // groups)
    viewed = jnp.swapaxes(viewed, axis_pos, 3)
    return viewed.reshape(outer_n, inner_n, rows_n, width)


def reference(stem_real, stem_imag, branch_real, branch_imag, orders):
    plane_real, plane_imag = multiply(stem_real, stem_imag, branch_real[0], branch_imag[0], orders[0])
    plane_real = swap_group(plane_real, N_INNER, 1)
    plane_imag = swap_group(plane_imag, N_INNER, 1)
    plane_real, plane_imag = multiply(plane_real, plane_imag, branch_real[1], branch_imag[1], orders[1])
    plane_real = swap_group(plane_real, N_OUTER, 0)
    plane_imag = swap_group(plane_imag, N_OUTER, 0)
    plane_real, plane_imag = multiply(plane_real, plane_imag, branch_real[2], branch_imag[2], orders[2])
    plane_real = swap_group(plane_real, N_INNER, 1)
    plane_imag = swap_group(plane_imag, N_INNER, 1)
    plane_real, plane_imag = multiply(plane_real, plane_imag, branch_real[3], branch_imag[3], orders[3])
    return plane_real, plane_imag
```

```python
import functools

import jax
import jax.numpy as jnp
from jax import lax
from jax.experimental import pallas as pl
from jax.experimental.pallas import tpu as pltpu
from jax.sharding import PartitionSpec as P

PRODUCTS = 4
LANES = 128


def halves(x):
    high = x.astype(jnp.bfloat16)
    return high, (x - high.astype(jnp.float32)).astype(jnp.bfloat16)


def dot(a, b):
    return jnp.dot(a, b, preferred_element_type=jnp.float32)


def tables_kernel(branch_real, branch_imag, orders, tables):
    width = branch_real.shape[1]
    places = lax.broadcasted_iota(jnp.int32, (width, width), 0)
    for p in range(PRODUCTS):
        selector = (places == orders[p, :][None, :]).astype(jnp.float32).astype(jnp.bfloat16)
        moved = []
        for m, plane in enumerate((branch_real, branch_imag)):
            high, low = halves(plane[p])
            high, low = dot(selector, high), dot(selector, low)
            tables[p, 2 * m] = high.astype(jnp.bfloat16)
            tables[p, 2 * m + 1] = low.astype(jnp.bfloat16)
            moved.append(high + low)
        high, low = halves(moved[0] + moved[1])
        tables[p, 4] = high
        tables[p, 5] = low


def pack_kernel(plane_real, plane_imag, packed):
    rows = plane_real.shape[2]
    for m, plane in enumerate((plane_real, plane_imag)):
        for q in range(4):
            packed[pl.ds(4 * m + q, rows, stride=8), :] = plane[0, 0, :, q * LANES:(q + 1) * LANES]


def unpack_kernel(packed, plane_real, plane_imag):
    rows = plane_real.shape[2]
    for m, plane in enumerate((plane_real, plane_imag)):
        for q in range(4):
            plane[0, 0, :, q * LANES:(q + 1) * LANES] = packed[pl.ds(4 * m + q, rows, stride=8), :]


def swap_groups(source, target, major):
    lane = lax.broadcasted_iota(jnp.int32, (16, LANES), 1)
    first_half = lane < 64
    even_group = (lane & 32) == 0
    for m in range(2):
        for q in range(4):
            for g in range(4):
                v = []
                for r in range(4):
                    s = 4 * g + r
                    rows = pl.ds(16 * s, 16) if major else pl.ds(s, 16, stride=16)
                    v.append(source[m, q, rows, :])
                for r in range(2):
                    a, b = v[r], v[r + 2]
                    c = pltpu.roll(jnp.where(first_half, b, a), 64, 1)
                    v[r] = jnp.where(first_half, a, c)
                    v[r + 2] = jnp.where(first_half, c, b)
                for r in (0, 2):
                    a, b = v[r], v[r + 1]
                    v[r] = jnp.where(even_group, a, pltpu.roll(b, 32, 1))
                    v[r + 1] = jnp.where(even_group, pltpu.roll(a, 96, 1), b)
                for t in range(4):
                    target[m, g, pl.ds((4 * q + t) * 16, 16), :] = v[t]


def multiply(real, imag, table):
    real_h, real_l = halves(real)
    imag_h, imag_l = halves(imag)
    sum_h, sum_l = halves(real + imag)
    width = real.shape[1]
    step = 256
    for n in range(width // step):
        columns = pl.ds(n * step, step)
        terms = []
        for k, (high, low) in enumerate(((real_h, real_l), (imag_h, imag_l), (sum_h, sum_l))):
            right_h, right_l = table[2 * k, :, columns], table[2 * k + 1, :, columns]
            terms.append(dot(high, right_h) + dot(high, right_l) + dot(low, right_h))
        out_real, out_imag = terms[0] - terms[1], terms[2] - terms[0] - terms[1]
        for j in range(step // LANES):
            tile = slice(j * LANES, (j + 1) * LANES)
            yield n * (step // LANES) + j, out_real[:, tile], out_imag[:, tile]


def stages_kernel(received, stored, sent, work, turned, tables, arrived):
    rows = received.shape[0] // 8
    fetches = [
        pltpu.make_async_copy(stored.at[p], tables.at[p], arrived.at[p]) for p in range(PRODUCTS)
    ]
    for fetch in fetches:
        fetch.start()

    def joined(m):
        return jnp.concatenate([turned[m, q] for q in range(4)], axis=1)

    for p in range(PRODUCTS):
        if p == 0:
            real, imag = (
                jnp.concatenate([received[pl.ds(4 * m + q, rows, stride=8), :] for q in range(4)], axis=1)
                for m in range(2)
            )
        else:
            swap_groups(work, turned, p == 1)
            real, imag = joined(0), joined(1)
        fetches[p].wait()
        for q, out_real, out_imag in multiply(real, imag, tables.at[p]):
            if p < PRODUCTS - 1:
                work[0, q] = out_real
                work[1, q] = out_imag
            else:
                sent[pl.ds(q, rows, stride=8), :] = out_real
                sent[pl.ds(4 + q, rows, stride=8), :] = out_imag


VMEM = pl.BlockSpec(memory_space=pltpu.VMEM)
HBM = pl.BlockSpec(memory_space=pltpu.HBM)


def call(kernel, out, specs, flops, scratch=(), limit=None):
    return pl.pallas_call(
        kernel,
        out_shape=out,
        in_specs=specs,
        out_specs=jax.tree.map(lambda _: VMEM, out),
        scratch_shapes=scratch,
        compiler_params=pltpu.CompilerParams(vmem_limit_bytes=limit),
        cost_estimate=pl.CostEstimate(flops=flops, bytes_accessed=2**21, transcendentals=0),
    )


def exchange(packed):
    pieces = packed.reshape(-1, 8, LANES)
    pieces = lax.all_to_all(pieces, ("inner", "outer"), split_axis=0, concat_axis=0, tiled=True)
    return pieces.reshape(packed.shape)


def on_device(stem_real, stem_imag, branch_real, branch_imag, orders):
    rows, width = stem_real.shape[2:]
    packed = jax.ShapeDtypeStruct((rows * 8, LANES), jnp.float32)
    plane = jax.ShapeDtypeStruct(stem_real.shape, jnp.float32)
    sent = call(pack_kernel, packed, [VMEM] * 2, 10**6, limit=4 * 2**20)(stem_real, stem_imag)
    tables = call(
        tables_kernel,
        jax.ShapeDtypeStruct((PRODUCTS, 6, width, width), jnp.bfloat16),
        [VMEM] * 3,
        2 * 16 * width**3,
        limit=32 * 2**20,
    )(branch_real, branch_imag, orders)
    received = exchange(sent)
    scratch = [
        pltpu.VMEM((2, 4, rows, LANES), jnp.float32),
        pltpu.VMEM((2, 4, rows, LANES), jnp.float32),
        pltpu.VMEM(tables.shape, tables.dtype),
        pltpu.SemaphoreType.DMA((PRODUCTS,)),
    ]
    flops = 2 * 36 * rows * width**2
    sent = call(stages_kernel, packed, [VMEM, HBM], flops, scratch, 40 * 2**20)(received, tables)
    received = exchange(sent)
    return tuple(call(unpack_kernel, (plane, plane), [VMEM], 10**6, limit=4 * 2**20)(received))


def solution(mesh):
    placed = (P("outer", "inner", None, None), P("outer", "inner", None, None), P(), P(), P())
    return jax.shard_map(
        on_device,
        mesh=mesh,
        in_specs=placed,
        out_specs=(P("outer", "inner", None, None), P("outer", "inner", None, None)),
        check_vma=False,
    )
```

```python
import functools

import jax
import jax.numpy as jnp
from jax import lax
from jax.experimental import pallas as pl
from jax.experimental.pallas import tpu as pltpu
from jax.sharding import PartitionSpec as P

PRODUCTS = 4
LANES = 128
PARTS = 4


def halves(x):
    high = x.astype(jnp.bfloat16)
    return high, (x - high.astype(jnp.float32)).astype(jnp.bfloat16)


def dot(a, b):
    return jnp.dot(a, b, preferred_element_type=jnp.float32)


def tables_kernel(branch_real, branch_imag, orders, tables):
    width = branch_real.shape[1]
    places = lax.broadcasted_iota(jnp.int32, (width, width), 0)
    for p in range(PRODUCTS):
        selector = (places == orders[p, :][None, :]).astype(jnp.float32).astype(jnp.bfloat16)
        moved = []
        for m, plane in enumerate((branch_real, branch_imag)):
            high, low = halves(plane[p])
            high, low = dot(selector, high), dot(selector, low)
            tables[p, 2 * m] = high.astype(jnp.bfloat16)
            tables[p, 2 * m + 1] = low.astype(jnp.bfloat16)
            moved.append(high + low)
        high, low = halves(moved[0] + moved[1])
        tables[p, 4] = high
        tables[p, 5] = low


def pack_kernel(plane_real, plane_imag, packed, planes, tiles, arrived, left):
    rows = plane_real.shape[2]
    part = rows // PARTS
    sources = (plane_real, plane_imag)
    fetches = [
        [
            pltpu.make_async_copy(
                source.at[0, 0, pl.ds(c * part, part)], planes.at[m, pl.ds(c * part, part)], arrived.at[m, c]
            )
            for m, source in enumerate(sources)
        ]
        for c in range(PARTS)
    ]
    for pair in fetches:
        for fetch in pair:
            fetch.start()
    leaves = []
    for c, pair in enumerate(fetches):
        for m, fetch in enumerate(pair):
            fetch.wait()
            for q in range(4):
                value = planes[m, pl.ds(c * part, part), q * LANES:(q + 1) * LANES]
                tiles[pl.ds(8 * c * part + 4 * m + q, part, stride=8), :] = value
        lines = pl.ds(8 * c * part, 8 * part)
        leaves.append(pltpu.make_async_copy(tiles.at[lines], packed.at[lines], left.at[c]))
        leaves[-1].start()
    for leave in leaves:
        leave.wait()


def unpack_kernel(packed, plane_real, plane_imag, planes, left):
    rows = plane_real.shape[2]
    part = rows // PARTS
    leaves = []
    for c in range(PARTS):
        for m, target in enumerate((plane_real, plane_imag)):
            for q in range(4):
                value = packed[pl.ds(8 * c * part + 4 * m + q, part, stride=8), :]
                planes[m, pl.ds(c * part, part), q * LANES:(q + 1) * LANES] = value
            leaves.append(
                pltpu.make_async_copy(
                    planes.at[m, pl.ds(c * part, part)], target.at[0, 0, pl.ds(c * part, part)], left.at[m, c]
                )
            )
            leaves[-1].start()
    for leave in leaves:
        leave.wait()


def swap_groups(source, target, major):
    lane = lax.broadcasted_iota(jnp.int32, (16, LANES), 1)
    first_half = lane < 64
    even_group = (lane & 32) == 0
    for m in range(2):
        for q in range(4):
            for g in range(4):
                v = []
                for r in range(4):
                    s = 4 * g + r
                    rows = pl.ds(24 * s, 16) if major else pl.ds(s, 16, stride=24)
                    v.append(source[m, q, rows, :])
                for r in range(2):
                    a, b = v[r], v[r + 2]
                    c = pltpu.roll(jnp.where(first_half, b, a), 64, 1)
                    v[r] = jnp.where(first_half, a, c)
                    v[r + 2] = jnp.where(first_half, c, b)
                for r in (0, 2):
                    a, b = v[r], v[r + 1]
                    v[r] = jnp.where(even_group, a, pltpu.roll(b, 32, 1))
                    v[r + 1] = jnp.where(even_group, pltpu.roll(a, 96, 1), b)
                for t in range(4):
                    target[m, g, pl.ds((4 * q + t) * 16, 16), :] = v[t]


def multiply(real, imag, table, left):
    for k, plane in enumerate((real, imag, real + imag)):
        left[2 * k], left[2 * k + 1] = halves(plane)
    width = real.shape[1]
    step = 256
    for n in range(width // step):
        columns = pl.ds(n * step, step)
        terms = []
        for k, (high, low) in enumerate(((left[0], left[1]), (left[2], left[3]), (left[4], left[5]))):
            right_h, right_l = table[2 * k, :, columns], table[2 * k + 1, :, columns]
            terms.append(dot(high, right_h) + dot(low, right_h) + dot(high, right_l))
        out_real, out_imag = terms[0] - terms[1], terms[2] - terms[0] - terms[1]
        for j in range(step // LANES):
            tile = slice(j * LANES, (j + 1) * LANES)
            yield n * (step // LANES) + j, out_real[:, tile], out_imag[:, tile]


def stages_kernel(received, stored, sent, work, turned, tables, left, arrived):
    rows = received.shape[0] // 8
    fetches = [
        pltpu.make_async_copy(stored.at[p], tables.at[p], arrived.at[p]) for p in range(PRODUCTS)
    ]
    for fetch in fetches:
        fetch.start()

    def joined(m):
        return jnp.concatenate([turned[m, q] for q in range(4)], axis=1)

    for p in range(PRODUCTS):
        if p == 0:
            real, imag = (
                jnp.concatenate([received[pl.ds(4 * m + q, rows, stride=8), :] for q in range(4)], axis=1)
                for m in range(2)
            )
        else:
            swap_groups(work, turned, p == 1)
            real, imag = joined(0), joined(1)
        fetches[p].wait()
        for q, out_real, out_imag in multiply(real, imag, tables.at[p], left):
            if p < PRODUCTS - 1:
                for u in range(16):
                    work[0, q, 24 * u:24 * u + 16] = out_real[16 * u:16 * u + 16]
                    work[1, q, 24 * u:24 * u + 16] = out_imag[16 * u:16 * u + 16]
            else:
                sent[pl.ds(q, rows, stride=8), :] = out_real
                sent[pl.ds(4 + q, rows, stride=8), :] = out_imag


VMEM = pl.BlockSpec(memory_space=pltpu.VMEM)
HBM = pl.BlockSpec(memory_space=pltpu.HBM)


def call(kernel, out, ins, outs, flops, scratch=(), limit=None):
    return pl.pallas_call(
        kernel,
        out_shape=out,
        in_specs=ins,
        out_specs=outs,
        scratch_shapes=scratch,
        compiler_params=pltpu.CompilerParams(vmem_limit_bytes=limit),
        cost_estimate=pl.CostEstimate(flops=flops, bytes_accessed=2**21, transcendentals=0),
    )


def exchange(packed):
    pieces = packed.reshape(-1, 8, LANES)
    pieces = lax.all_to_all(pieces, ("inner", "outer"), split_axis=0, concat_axis=0, tiled=True)
    return pieces.reshape(packed.shape)


def on_device(stem_real, stem_imag, branch_real, branch_imag, orders):
    rows, width = stem_real.shape[2:]
    packed = jax.ShapeDtypeStruct((rows * 8, LANES), jnp.float32)
    plane = jax.ShapeDtypeStruct(stem_real.shape, jnp.float32)
    planes = pltpu.VMEM((2, rows, width), jnp.float32)
    tiled = pltpu.VMEM((2, 4, rows, LANES), jnp.float32)
    dma = pltpu.SemaphoreType.DMA
    scratch = [planes, pltpu.VMEM(packed.shape, packed.dtype), dma((2, PARTS)), dma((PARTS,))]
    sent = call(pack_kernel, packed, [HBM] * 2, HBM, 10**6, scratch)(stem_real, stem_imag)
    stored = jax.ShapeDtypeStruct((PRODUCTS, 6, width, width), jnp.bfloat16)
    stored = call(tables_kernel, stored, [VMEM] * 3, VMEM, 32 * width**3, (), 32 * 2**20)(
        branch_real, branch_imag, orders
    )
    received = exchange(sent)
    scratch = [
        pltpu.VMEM((2, 4, 384, LANES), jnp.float32),
        tiled,
        pltpu.VMEM(stored.shape, stored.dtype),
        pltpu.VMEM((6, rows, width), stored.dtype),
        dma((PRODUCTS,)),
    ]
    flops = 2 * 36 * rows * width**2
    sent = call(stages_kernel, packed, [VMEM, HBM], VMEM, flops, scratch, 40 * 2**20)(received, stored)
    received = exchange(sent)
    scratch = [planes, dma((2, PARTS))]
    return tuple(
        call(unpack_kernel, (plane, plane), [VMEM], (HBM, HBM), 10**6, scratch, 4 * 2**20)(received)
    )


def solution(mesh):
    placed = (P("outer", "inner", None, None), P("outer", "inner", None, None), P(), P(), P())
    return jax.shard_map(
        on_device,
        mesh=mesh,
        in_specs=placed,
        out_specs=(P("outer", "inner", None, None), P("outer", "inner", None, None)),
        check_vma=False,
    )
```

```python
import functools

import jax
import jax.numpy as jnp
from jax import lax
from jax.experimental import pallas as pl
from jax.experimental.pallas import tpu as pltpu
from jax.sharding import PartitionSpec as P

PRODUCTS = 4
LANES = 128
PARTS = 4


def halves(x):
    high = x.astype(jnp.bfloat16)
    return high, (x - high.astype(jnp.float32)).astype(jnp.bfloat16)


def dot(a, b):
    return jnp.dot(a, b, preferred_element_type=jnp.float32)


def spans():
    counts = [2] + [6] * (PRODUCTS - 1)
    return [pl.ds(sum(counts[:p]), count) for p, count in enumerate(counts)]


def tables_kernel(branch_real, branch_imag, orders, first, stored):
    width = branch_real.shape[1]
    places = lax.broadcasted_iota(jnp.int32, (width, width), 0)
    for p, span in enumerate(spans()):
        selector = (places == orders[p, :][None, :]).astype(jnp.float32).astype(jnp.bfloat16)
        last = span.start + span.size
        moved = []
        for m, plane in enumerate((branch_real, branch_imag)):
            high, low = halves(plane[p])
            high, low = dot(selector, high), dot(selector, low)
            table, place = (first, 2 * m) if p == 0 else (stored, span.start + 2 * m)
            table[place] = high.astype(jnp.bfloat16)
            table[place + 1] = low.astype(jnp.bfloat16)
            moved.append(high + low)
        high, low = halves(moved[0] + moved[1])
        stored[last - 2] = high
        stored[last - 1] = low


def pack_kernel(plane_real, plane_imag, packed, planes, tiles, arrived, left):
    rows = plane_real.shape[2]
    part = rows // PARTS
    sources = (plane_real, plane_imag)
    fetches = [
        [
            pltpu.make_async_copy(
                source.at[0, 0, pl.ds(c * part, part)], planes.at[m, pl.ds(c * part, part)], arrived.at[m, c]
            )
            for m, source in enumerate(sources)
        ]
        for c in range(PARTS)
    ]
    for pair in fetches:
        for fetch in pair:
            fetch.start()
    leaves = []
    for c, pair in enumerate(fetches):
        for m, fetch in enumerate(pair):
            fetch.wait()
            for q in range(4):
                value = planes[m, pl.ds(c * part, part), q * LANES:(q + 1) * LANES]
                tiles[pl.ds(8 * c * part + 4 * m + q, part, stride=8), :] = value
        lines = pl.ds(8 * c * part, 8 * part)
        leaves.append(pltpu.make_async_copy(tiles.at[lines], packed.at[lines], left.at[c]))
        leaves[-1].start()
    for leave in leaves:
        leave.wait()


def unpack_kernel(packed, plane_real, plane_imag, planes, left):
    rows = plane_real.shape[2]
    part = rows // PARTS
    leaves = []
    for c in range(PARTS):
        for m, target in enumerate((plane_real, plane_imag)):
            for q in range(4):
                value = packed[pl.ds(8 * c * part + 4 * m + q, part, stride=8), :]
                planes[m, pl.ds(c * part, part), q * LANES:(q + 1) * LANES] = value
            leaves.append(
                pltpu.make_async_copy(
                    planes.at[m, pl.ds(c * part, part)], target.at[0, 0, pl.ds(c * part, part)], left.at[m, c]
                )
            )
            leaves[-1].start()
    for leave in leaves:
        leave.wait()


def swap_groups(source, target, major):
    lane = lax.broadcasted_iota(jnp.int32, (16, LANES), 1)
    first_half = lane < 64
    even_group = (lane & 32) == 0
    for m in range(2):
        for q in range(4):
            for g in range(4):
                v = []
                for r in range(4):
                    s = 4 * g + r
                    rows = pl.ds(24 * s, 16) if major else pl.ds(s, 16, stride=24)
                    v.append(source[m, q, rows, :])
                for r in range(2):
                    a, b = v[r], v[r + 2]
                    c = pltpu.roll(jnp.where(first_half, b, a), 64, 1)
                    v[r] = jnp.where(first_half, a, c)
                    v[r + 2] = jnp.where(first_half, c, b)
                for r in (0, 2):
                    a, b = v[r], v[r + 1]
                    v[r] = jnp.where(even_group, a, pltpu.roll(b, 32, 1))
                    v[r + 1] = jnp.where(even_group, pltpu.roll(a, 96, 1), b)
                for t in range(4):
                    target[m, g, pl.ds((4 * q + t) * 16, 16), :] = v[t]


def multiply(real, imag, tables, left, ready):
    for k, plane in enumerate((real, imag, real + imag)):
        left[2 * k], left[2 * k + 1] = halves(plane)
    width = real.shape[1]
    step = 256
    for n in range(width // step):
        columns = slice(n * step, (n + 1) * step)
        terms = []
        for k in range(3):
            if n == 0:
                ready(k)
            high, low = left[2 * k], left[2 * k + 1]
            right_h, right_l = (table[place, :, columns] for table, place in tables[2 * k:2 * k + 2])
            terms.append(dot(high, right_h) + dot(low, right_h) + dot(high, right_l))
        out_real, out_imag = terms[0] - terms[1], terms[2] - terms[0] - terms[1]
        for j in range(step // LANES):
            tile = slice(j * LANES, (j + 1) * LANES)
            yield n * (step // LANES) + j, out_real[:, tile], out_imag[:, tile]


def stages_kernel(received, first, stored, sent, work, turned, later, left, arrived):
    rows = received.shape[0] // 8
    fetches = [
        pltpu.make_async_copy(stored.at[span], later.at[span], arrived.at[p]) for p, span in enumerate(spans())
    ]
    for p, fetch in enumerate(fetches):
        fetch.start(priority=min(p, 1))

    for p, span in enumerate(spans()):
        if p == 0:
            real, imag = (
                jnp.concatenate([received[pl.ds(4 * m + q, rows, stride=8), :] for q in range(4)], axis=1)
                for m in range(2)
            )
        else:
            swap_groups(work, turned, p == 1)
            real, imag = (jnp.concatenate([turned[m, q] for q in range(4)], axis=1) for m in range(2))
        tables = [(later, span.start + j) for j in range(span.size)]
        if p == 0:
            tables = [(first, j) for j in range(4)] + tables

        def ready(k, p=p):
            if k == (2 if p == 0 else 0):
                fetches[p].wait()

        for q, out_real, out_imag in multiply(real, imag, tables, left, ready):
            if p < PRODUCTS - 1:
                for u in range(16):
                    work[0, q, 24 * u:24 * u + 16] = out_real[16 * u:16 * u + 16]
                    work[1, q, 24 * u:24 * u + 16] = out_imag[16 * u:16 * u + 16]
            else:
                sent[pl.ds(q, rows, stride=8), :] = out_real
                sent[pl.ds(4 + q, rows, stride=8), :] = out_imag


VMEM = pl.BlockSpec(memory_space=pltpu.VMEM)
HBM = pl.BlockSpec(memory_space=pltpu.HBM)


def call(kernel, out, ins, outs, flops, scratch=(), limit=None):
    return pl.pallas_call(
        kernel,
        out_shape=out,
        in_specs=ins,
        out_specs=outs,
        scratch_shapes=scratch,
        compiler_params=pltpu.CompilerParams(vmem_limit_bytes=limit),
        cost_estimate=pl.CostEstimate(flops=flops, bytes_accessed=2**21, transcendentals=0),
    )


def exchange(packed):
    pieces = packed.reshape(-1, 8, LANES)
    pieces = lax.all_to_all(pieces, ("inner", "outer"), split_axis=0, concat_axis=0, tiled=True)
    return pieces.reshape(packed.shape)


def on_device(stem_real, stem_imag, branch_real, branch_imag, orders):
    rows, width = stem_real.shape[2:]
    packed = jax.ShapeDtypeStruct((rows * 8, LANES), jnp.float32)
    plane = jax.ShapeDtypeStruct(stem_real.shape, jnp.float32)
    planes = pltpu.VMEM((2, rows, width), jnp.float32)
    tiled = pltpu.VMEM((2, 4, rows, LANES), jnp.float32)
    dma = pltpu.SemaphoreType.DMA
    scratch = [planes, pltpu.VMEM(packed.shape, packed.dtype), dma((2, PARTS)), dma((PARTS,))]
    sent = call(pack_kernel, packed, [HBM] * 2, HBM, 10**6, scratch)(stem_real, stem_imag)
    first = jax.ShapeDtypeStruct((4, width, width), jnp.bfloat16)
    stored = jax.ShapeDtypeStruct((6 * PRODUCTS - 4, width, width), jnp.bfloat16)
    first, stored = call(
        tables_kernel, (first, stored), [VMEM] * 3, (VMEM, VMEM), 32 * width**3, (), 32 * 2**20
    )(branch_real, branch_imag, orders)
    received = exchange(sent)
    scratch = [
        pltpu.VMEM((2, 4, 384, LANES), jnp.float32),
        tiled,
        pltpu.VMEM(stored.shape, stored.dtype),
        pltpu.VMEM((6, rows, width), stored.dtype),
        dma((PRODUCTS,)),
    ]
    flops = 2 * 36 * rows * width**2
    sent = call(stages_kernel, packed, [VMEM, VMEM, HBM], VMEM, flops, scratch, 40 * 2**20)(
        received, first, stored
    )
    received = exchange(sent)
    scratch = [planes, dma((2, PARTS))]
    return tuple(
        call(unpack_kernel, (plane, plane), [VMEM], (HBM, HBM), 10**6, scratch, 4 * 2**20)(received)
    )


def solution(mesh):
    placed = (P("outer", "inner", None, None), P("outer", "inner", None, None), P(), P(), P())
    return jax.shard_map(
        on_device,
        mesh=mesh,
        in_specs=placed,
        out_specs=(P("outer", "inner", None, None), P("outer", "inner", None, None)),
        check_vma=False,
    )
```

```python
import functools

import jax
import jax.numpy as jnp
from jax import lax
from jax.experimental import pallas as pl
from jax.experimental.pallas import tpu as pltpu
from jax.sharding import Mesh
from jax.sharding import PartitionSpec as P

PRODUCTS = 4
LANES = 128
PARTS = 4
ORDER = ("zhi", "zlo", "y", "x", "core")


def halves(x):
    high = x.astype(jnp.bfloat16)
    return high, (x - high.astype(jnp.float32)).astype(jnp.bfloat16)


def dot(a, b):
    return jnp.dot(a, b, preferred_element_type=jnp.float32)


def spans():
    counts = [2] + [6] * (PRODUCTS - 1)
    return [pl.ds(sum(counts[:p]), count) for p, count in enumerate(counts)]


def tables_kernel(branch_real, branch_imag, orders, first, stored):
    width = branch_real.shape[1]
    places = lax.broadcasted_iota(jnp.int32, (width, width), 0)
    for p, span in enumerate(spans()):
        selector = (places == orders[p, :][None, :]).astype(jnp.float32).astype(jnp.bfloat16)
        last = span.start + span.size
        moved = []
        for m, plane in enumerate((branch_real, branch_imag)):
            high, low = halves(plane[p])
            high, low = dot(selector, high), dot(selector, low)
            table, place = (first, 2 * m) if p == 0 else (stored, span.start + 2 * m)
            table[place] = high.astype(jnp.bfloat16)
            table[place + 1] = low.astype(jnp.bfloat16)
            moved.append(high + low)
        high, low = halves(moved[0] + moved[1])
        stored[last - 2] = high
        stored[last - 1] = low


def pack_kernel(plane_real, plane_imag, packed, planes, tiles, arrived, left):
    rows = plane_real.shape[2]
    part = rows // PARTS
    sources = (plane_real, plane_imag)
    fetches = [
        [
            pltpu.make_async_copy(
                source.at[0, 0, pl.ds(c * part, part)], planes.at[m, pl.ds(c * part, part)], arrived.at[m, c]
            )
            for m, source in enumerate(sources)
        ]
        for c in range(PARTS)
    ]
    for pair in fetches:
        for fetch in pair:
            fetch.start()
    leaves = []
    for c, pair in enumerate(fetches):
        for m, fetch in enumerate(pair):
            fetch.wait()
            for q in range(4):
                value = planes[m, pl.ds(c * part, part), q * LANES:(q + 1) * LANES]
                tiles[pl.ds(8 * c * part + 4 * m + q, part, stride=8), :] = value
        lines = pl.ds(8 * c * part, 8 * part)
        leaves.append(pltpu.make_async_copy(tiles.at[lines], packed.at[lines], left.at[c]))
        leaves[-1].start()
    for leave in leaves:
        leave.wait()


def unpack_kernel(packed, plane_real, plane_imag, planes, left):
    rows = plane_real.shape[2]
    part = rows // PARTS
    leaves = []
    for c in range(PARTS):
        for m, target in enumerate((plane_real, plane_imag)):
            for q in range(4):
                value = packed[pl.ds(8 * c * part + 4 * m + q, part, stride=8), :]
                planes[m, pl.ds(c * part, part), q * LANES:(q + 1) * LANES] = value
            leaves.append(
                pltpu.make_async_copy(
                    planes.at[m, pl.ds(c * part, part)], target.at[0, 0, pl.ds(c * part, part)], left.at[m, c]
                )
            )
            leaves[-1].start()
    for leave in leaves:
        leave.wait()


def place(inner):
    return 128 * (inner // 2 % 2) + 2 * (inner // 4) + inner % 2


def swap_groups(source, target, first, last):
    lane = lax.broadcasted_iota(jnp.int32, (16, LANES), 1)
    first_half = lane < 64
    even_group = (lane & 32) == 0
    for m in range(2):
        for q in range(4):
            for g in range(4):
                v = []
                for r in range(4):
                    s = 4 * g + r
                    rows = pl.ds(place(s), 16, stride=8) if first else pl.ds(s, 16, stride=24)
                    v.append(source[m, q, rows, :])
                for r in range(2):
                    a, b = v[r], v[r + 2]
                    c = pltpu.roll(jnp.where(first_half, b, a), 64, 1)
                    v[r] = jnp.where(first_half, a, c)
                    v[r + 2] = jnp.where(first_half, c, b)
                for r in (0, 2):
                    a, b = v[r], v[r + 1]
                    v[r] = jnp.where(even_group, a, pltpu.roll(b, 32, 1))
                    v[r + 1] = jnp.where(even_group, pltpu.roll(a, 96, 1), b)
                for t in range(4):
                    s = 4 * q + t
                    rows = pl.ds(place(s), 16, stride=8) if last else pl.ds(16 * s, 16)
                    target[m, g, rows, :] = v[t]


def multiply(real, imag, tables, left, ready):
    rows = real.shape[0]
    for k, plane in enumerate((real, imag, real + imag)):
        left[k, :rows], left[k, rows:] = halves(plane)
    width = real.shape[1]
    step = 256
    for n in range(width // step):
        columns = slice(n * step, (n + 1) * step)
        terms = []
        for k in range(3):
            if n == 0:
                ready(k)
            right_h, right_l = (table[place, :, columns] for table, place in tables[2 * k:2 * k + 2])
            both = dot(left[k], right_h)
            terms.append(both[:rows] + both[rows:] + dot(left[k, :rows], right_l))
        out_real, out_imag = terms[0] - terms[1], terms[2] - terms[0] - terms[1]
        for j in range(step // LANES):
            tile = slice(j * LANES, (j + 1) * LANES)
            yield n * (step // LANES) + j, out_real[:, tile], out_imag[:, tile]


def stages_kernel(received, first, stored, sent, work, turned, later, left, arrived):
    rows = received.shape[0] // 8
    fetches = [
        pltpu.make_async_copy(stored.at[span], later.at[span], arrived.at[p]) for p, span in enumerate(spans())
    ]
    for p, fetch in enumerate(fetches):
        fetch.start(priority=min(p, 1))

    for p, span in enumerate(spans()):
        if p == 0:
            real, imag = (
                jnp.concatenate([received[pl.ds(4 * m + q, rows, stride=8), :] for q in range(4)], axis=1)
                for m in range(2)
            )
        else:
            swap_groups(work, turned, p == 1, p == PRODUCTS - 1)
            real, imag = (jnp.concatenate([turned[m, q] for q in range(4)], axis=1) for m in range(2))
        tables = [(later, span.start + j) for j in range(span.size)]
        if p == 0:
            tables = [(first, j) for j in range(4)] + tables

        def ready(k, p=p):
            if k == (2 if p == 0 else 0):
                fetches[p].wait()

        for q, out_real, out_imag in multiply(real, imag, tables, left, ready):
            if p == 0:
                work[0, q, :rows] = out_real
                work[1, q, :rows] = out_imag
            elif p < PRODUCTS - 1:
                for u in range(16):
                    work[0, q, 24 * u:24 * u + 16] = out_real[16 * u:16 * u + 16]
                    work[1, q, 24 * u:24 * u + 16] = out_imag[16 * u:16 * u + 16]
            else:
                sent[pl.ds(q, rows, stride=8), :] = out_real
                sent[pl.ds(4 + q, rows, stride=8), :] = out_imag


VMEM = pl.BlockSpec(memory_space=pltpu.VMEM)
HBM = pl.BlockSpec(memory_space=pltpu.HBM)


def call(kernel, out, ins, outs, flops, scratch=(), limit=None):
    return pl.pallas_call(
        kernel,
        out_shape=out,
        in_specs=ins,
        out_specs=outs,
        scratch_shapes=scratch,
        compiler_params=pltpu.CompilerParams(vmem_limit_bytes=limit),
        cost_estimate=pl.CostEstimate(flops=flops, bytes_accessed=2**21, transcendentals=0),
    )


def exchange(packed):
    pieces = packed.reshape(-1, 8, LANES)
    pieces = lax.all_to_all(pieces, ORDER, split_axis=0, concat_axis=0, tiled=True)
    return pieces.reshape(packed.shape)


def on_device(stem_real, stem_imag, branch_real, branch_imag, orders):
    rows, width = stem_real.shape[2:]
    packed = jax.ShapeDtypeStruct((rows * 8, LANES), jnp.float32)
    plane = jax.ShapeDtypeStruct(stem_real.shape, jnp.float32)
    planes = pltpu.VMEM((2, rows, width), jnp.float32)
    tiled = pltpu.VMEM((2, 4, rows, LANES), jnp.float32)
    dma = pltpu.SemaphoreType.DMA
    scratch = [planes, pltpu.VMEM(packed.shape, packed.dtype), dma((2, PARTS)), dma((PARTS,))]
    sent = call(pack_kernel, packed, [HBM] * 2, HBM, 10**6, scratch)(stem_real, stem_imag)
    first = jax.ShapeDtypeStruct((4, width, width), jnp.bfloat16)
    stored = jax.ShapeDtypeStruct((6 * PRODUCTS - 4, width, width), jnp.bfloat16)
    first, stored = call(
        tables_kernel, (first, stored), [VMEM] * 3, (VMEM, VMEM), 32 * width**3, (), 32 * 2**20
    )(branch_real, branch_imag, orders)
    received = exchange(sent)
    scratch = [
        pltpu.VMEM((2, 4, 384, LANES), jnp.float32),
        tiled,
        pltpu.VMEM(stored.shape, stored.dtype),
        pltpu.VMEM((3, 2 * rows, width), stored.dtype),
        dma((PRODUCTS,)),
    ]
    flops = 2 * 36 * rows * width**2
    sent = call(stages_kernel, packed, [VMEM, VMEM, HBM], VMEM, flops, scratch, 40 * 2**20)(
        received, first, stored
    )
    received = exchange(sent)
    scratch = [planes, dma((2, PARTS))]
    return tuple(
        call(unpack_kernel, (plane, plane), [VMEM], (HBM, HBM), 10**6, scratch, 4 * 2**20)(received)
    )


def solution(mesh):
    chips = Mesh(mesh.devices.reshape(4, 4, 4, 2, 2), ("zlo", "y", "x", "zhi", "core"))
    stem = P(("zlo", "y"), ("x", "zhi", "core"), None, None)
    return jax.shard_map(
        on_device,
        mesh=chips,
        in_specs=(stem, stem, P(), P(), P()),
        out_specs=(stem, stem),
        check_vma=False,
    )
```

```python
import functools

import jax
import jax.numpy as jnp
from jax import lax
from jax.experimental import pallas as pl
from jax.experimental.pallas import tpu as pltpu
from jax.sharding import Mesh
from jax.sharding import PartitionSpec as P

PRODUCTS = 4
LANES = 128
PARTS = 4
ORDER = ("zhi", "zlo", "y", "x", "core")


def halves(x):
    high = x.astype(jnp.bfloat16)
    return high, (x - high.astype(jnp.float32)).astype(jnp.bfloat16)


def dot(a, b):
    return jnp.dot(a, b, preferred_element_type=jnp.float32)


def spans():
    counts = [0] + [4] * (PRODUCTS - 1)
    return [pl.ds(sum(counts[:p]), count) for p, count in enumerate(counts)]


def tables_kernel(branch_real, branch_imag, orders, first, stored):
    width = branch_real.shape[1]
    places = lax.broadcasted_iota(jnp.int32, (width, width), 0)
    for p, span in enumerate(spans()):
        selector = (places == orders[p, :][None, :]).astype(jnp.float32).astype(jnp.bfloat16)
        for m, plane in enumerate((branch_real, branch_imag)):
            high, low = halves(plane[p])
            high, low = dot(selector, high), dot(selector, low)
            table, place = (first, 2 * m) if p == 0 else (stored, span.start + 2 * m)
            table[place] = high.astype(jnp.bfloat16)
            table[place + 1] = low.astype(jnp.bfloat16)


def pack_kernel(plane_real, plane_imag, packed, planes, tiles, arrived, left):
    rows = plane_real.shape[2]
    part = rows // PARTS
    sources = (plane_real, plane_imag)
    fetches = [
        [
            pltpu.make_async_copy(
                source.at[0, 0, pl.ds(c * part, part)], planes.at[m, pl.ds(c * part, part)], arrived.at[m, c]
            )
            for m, source in enumerate(sources)
        ]
        for c in range(PARTS)
    ]
    for pair in fetches:
        for fetch in pair:
            fetch.start()
    leaves = []
    for c, pair in enumerate(fetches):
        for m, fetch in enumerate(pair):
            fetch.wait()
            for q in range(4):
                value = planes[m, pl.ds(c * part, part), q * LANES:(q + 1) * LANES]
                tiles[pl.ds(8 * c * part + 4 * m + q, part, stride=8), :] = value
        lines = pl.ds(8 * c * part, 8 * part)
        leaves.append(pltpu.make_async_copy(tiles.at[lines], packed.at[lines], left.at[c]))
        leaves[-1].start()
    for leave in leaves:
        leave.wait()


def unpack_kernel(packed, plane_real, plane_imag, planes, left):
    rows = plane_real.shape[2]
    part = rows // PARTS
    leaves = []
    for c in range(PARTS):
        for m, target in enumerate((plane_real, plane_imag)):
            for q in range(4):
                value = packed[pl.ds(8 * c * part + 4 * m + q, part, stride=8), :]
                planes[m, pl.ds(c * part, part), q * LANES:(q + 1) * LANES] = value
            leaves.append(
                pltpu.make_async_copy(
                    planes.at[m, pl.ds(c * part, part)], target.at[0, 0, pl.ds(c * part, part)], left.at[m, c]
                )
            )
            leaves[-1].start()
    for leave in leaves:
        leave.wait()


def place(inner):
    return 128 * (inner // 2 % 2) + 2 * (inner // 4) + inner % 2


def swap_groups(source, target, first, last):
    lane = lax.broadcasted_iota(jnp.int32, (16, LANES), 1)
    first_half = lane < 64
    even_group = (lane & 32) == 0
    for m in range(2):
        for q in range(4):
            for g in range(4):
                v = []
                for r in range(4):
                    s = 4 * g + r
                    rows = pl.ds(place(s), 16, stride=8) if first else pl.ds(s, 16, stride=24)
                    v.append(source[m, q, rows, :])
                for r in range(2):
                    a, b = v[r], v[r + 2]
                    c = pltpu.roll(jnp.where(first_half, b, a), 64, 1)
                    v[r] = jnp.where(first_half, a, c)
                    v[r + 2] = jnp.where(first_half, c, b)
                for r in (0, 2):
                    a, b = v[r], v[r + 1]
                    v[r] = jnp.where(even_group, a, pltpu.roll(b, 32, 1))
                    v[r + 1] = jnp.where(even_group, pltpu.roll(a, 96, 1), b)
                for t in range(4):
                    s = 4 * q + t
                    rows = pl.ds(place(s), 16, stride=8) if last else pl.ds(16 * s, 16)
                    target[m, g, rows, :] = v[t]


def multiply(real, imag, tables, left, ready):
    rows = real.shape[0]
    for k, plane in enumerate((real, imag, real + imag)):
        left[k, :rows], left[k, rows:] = halves(plane)
    width = real.shape[1]
    step = 256
    for n in range(width // step):
        columns = slice(n * step, (n + 1) * step)
        terms = []
        for k in range(3):
            if n == 0:
                ready(k)
            right_h, right_l = (table[place, :, columns] for table, place in tables[2 * k:2 * k + 2])
            both = dot(left[k], right_h)
            terms.append(both[:rows] + both[rows:] + dot(left[k, :rows], right_l))
        out_real, out_imag = terms[0] - terms[1], terms[2] - terms[0] - terms[1]
        for j in range(step // LANES):
            tile = slice(j * LANES, (j + 1) * LANES)
            yield n * (step // LANES) + j, out_real[:, tile], out_imag[:, tile]


def stages_kernel(received, first, stored, sent, work, turned, later, left, sums, arrived):
    rows = received.shape[0] // 8
    fetches = [
        pltpu.make_async_copy(stored.at[span], later.at[span], arrived.at[p - 1]) for p, span in enumerate(spans()) if p > 0
    ]
    for fetch in fetches:
        fetch.start()

    for p, span in enumerate(spans()):
        if p == 0:
            real, imag = (
                jnp.concatenate([received[pl.ds(4 * m + q, rows, stride=8), :] for q in range(4)], axis=1)
                for m in range(2)
            )
        else:
            swap_groups(work, turned, p == 1, p == PRODUCTS - 1)
            real, imag = (jnp.concatenate([turned[m, q] for q in range(4)], axis=1) for m in range(2))
        tables = [(later, span.start + j) for j in range(span.size)]
        if p == 0:
            tables = [(first, j) for j in range(4)]
        if len(tables) == 4:
            tables += [(sums, 0), (sums, 1)]

        def ready(k, p=p, tables=tables):
            if k == 0 and p > 0:
                fetches[p - 1].wait()
            if k == 1 and tables[4][0] is sums:
                parts = [table[place].astype(jnp.float32) for table, place in tables[:4]]
                sums[0], sums[1] = halves((parts[0] + parts[1]) + (parts[2] + parts[3]))

        for q, out_real, out_imag in multiply(real, imag, tables, left, ready):
            if p == 0:
                work[0, q, :rows] = out_real
                work[1, q, :rows] = out_imag
            elif p < PRODUCTS - 1:
                for u in range(16):
                    work[0, q, 24 * u:24 * u + 16] = out_real[16 * u:16 * u + 16]
                    work[1, q, 24 * u:24 * u + 16] = out_imag[16 * u:16 * u + 16]
            else:
                sent[pl.ds(q, rows, stride=8), :] = out_real
                sent[pl.ds(4 + q, rows, stride=8), :] = out_imag


VMEM = pl.BlockSpec(memory_space=pltpu.VMEM)
HBM = pl.BlockSpec(memory_space=pltpu.HBM)


def call(kernel, out, ins, outs, flops, scratch=(), limit=None):
    return pl.pallas_call(
        kernel,
        out_shape=out,
        in_specs=ins,
        out_specs=outs,
        scratch_shapes=scratch,
        compiler_params=pltpu.CompilerParams(vmem_limit_bytes=limit),
        cost_estimate=pl.CostEstimate(flops=flops, bytes_accessed=2**21, transcendentals=0),
    )


def exchange(packed):
    pieces = packed.reshape(-1, 8, LANES)
    pieces = lax.all_to_all(pieces, ORDER, split_axis=0, concat_axis=0, tiled=True)
    return pieces.reshape(packed.shape)


def on_device(stem_real, stem_imag, branch_real, branch_imag, orders):
    rows, width = stem_real.shape[2:]
    packed = jax.ShapeDtypeStruct((rows * 8, LANES), jnp.float32)
    plane = jax.ShapeDtypeStruct(stem_real.shape, jnp.float32)
    planes = pltpu.VMEM((2, rows, width), jnp.float32)
    tiled = pltpu.VMEM((2, 4, rows, LANES), jnp.float32)
    dma = pltpu.SemaphoreType.DMA
    scratch = [planes, pltpu.VMEM(packed.shape, packed.dtype), dma((2, PARTS)), dma((PARTS,))]
    sent = call(pack_kernel, packed, [HBM] * 2, HBM, 10**6, scratch)(stem_real, stem_imag)
    first = jax.ShapeDtypeStruct((4, width, width), jnp.bfloat16)
    stored = jax.ShapeDtypeStruct((4 * PRODUCTS - 4, width, width), jnp.bfloat16)
    first, stored = call(
        tables_kernel, (first, stored), [VMEM] * 3, (VMEM, VMEM), 32 * width**3, (), 32 * 2**20
    )(branch_real, branch_imag, orders)
    received = exchange(sent)
    scratch = [
        pltpu.VMEM((2, 4, 384, LANES), jnp.float32),
        tiled,
        pltpu.VMEM(stored.shape, stored.dtype),
        pltpu.VMEM((3, 2 * rows, width), stored.dtype),
        pltpu.VMEM((2, width, width), stored.dtype),
        dma((PRODUCTS - 1,)),
    ]
    flops = 2 * 36 * rows * width**2
    sent = call(stages_kernel, packed, [VMEM, VMEM, HBM], VMEM, flops, scratch, 40 * 2**20)(
        received, first, stored
    )
    received = exchange(sent)
    scratch = [planes, dma((2, PARTS))]
    return tuple(
        call(unpack_kernel, (plane, plane), [VMEM], (HBM, HBM), 10**6, scratch, 4 * 2**20)(received)
    )


def solution(mesh):
    chips = Mesh(mesh.devices.reshape(4, 4, 4, 2, 2), ("zlo", "y", "x", "zhi", "core"))
    stem = P(("zlo", "y"), ("x", "zhi", "core"), None, None)
    return jax.shard_map(
        on_device,
        mesh=chips,
        in_specs=(stem, stem, P(), P(), P()),
        out_specs=(stem, stem),
        check_vma=False,
    )
```

```python
import functools

import jax
import jax.numpy as jnp
from jax import lax
from jax.experimental import pallas as pl
from jax.experimental.pallas import tpu as pltpu
from jax.sharding import Mesh
from jax.sharding import PartitionSpec as P

PRODUCTS = 4
LANES = 128
PARTS = 4
ORDER = ("x", "zhi", "zlo", "y", "core")


def halves(x):
    high = x.astype(jnp.bfloat16)
    return high, (x - high.astype(jnp.float32)).astype(jnp.bfloat16)


def dot(a, b):
    return jnp.dot(a, b, preferred_element_type=jnp.float32)


def spans():
    counts = [2] + [6] * (PRODUCTS - 1)
    return [pl.ds(sum(counts[:p]), count) for p, count in enumerate(counts)]


def tables_kernel(branch_real, branch_imag, orders, first, stored):
    width = branch_real.shape[1]
    places = lax.broadcasted_iota(jnp.int32, (width, width), 0)
    for p, span in enumerate(spans()):
        selector = (places == orders[p, :][None, :]).astype(jnp.float32).astype(jnp.bfloat16)
        last = span.start + span.size
        moved = []
        for m, plane in enumerate((branch_real, branch_imag)):
            high, low = halves(plane[p])
            high, low = dot(selector, high), dot(selector, low)
            table, place = (first, 2 * m) if p == 0 else (stored, span.start + 2 * m)
            table[place] = high.astype(jnp.bfloat16)
            table[place + 1] = low.astype(jnp.bfloat16)
            moved.append(high + low)
        high, low = halves(moved[0] + moved[1])
        stored[last - 2] = high
        stored[last - 1] = low


def pack_kernel(plane_real, plane_imag, packed, planes, tiles, arrived, left):
    rows = plane_real.shape[2]
    part = rows // PARTS
    sources = (plane_real, plane_imag)
    fetches = [
        [
            pltpu.make_async_copy(
                source.at[0, 0, pl.ds(c * part, part)], planes.at[m, pl.ds(c * part, part)], arrived.at[m, c]
            )
            for m, source in enumerate(sources)
        ]
        for c in range(PARTS)
    ]
    for pair in fetches:
        for fetch in pair:
            fetch.start()
    leaves = []
    for c, pair in enumerate(fetches):
        for m, fetch in enumerate(pair):
            fetch.wait()
            for q in range(4):
                value = planes[m, pl.ds(c * part, part), q * LANES:(q + 1) * LANES]
                tiles[pl.ds(8 * c * part + 4 * m + q, part, stride=8), :] = value
        lines = pl.ds(8 * c * part, 8 * part)
        leaves.append(pltpu.make_async_copy(tiles.at[lines], packed.at[lines], left.at[c]))
        leaves[-1].start()
    for leave in leaves:
        leave.wait()


def unpack_kernel(packed, plane_real, plane_imag, planes, left):
    rows = plane_real.shape[2]
    part = rows // PARTS
    leaves = []
    for c in range(PARTS):
        for m, target in enumerate((plane_real, plane_imag)):
            for q in range(4):
                value = packed[pl.ds(8 * c * part + 4 * m + q, part, stride=8), :]
                planes[m, pl.ds(c * part, part), q * LANES:(q + 1) * LANES] = value
            leaves.append(
                pltpu.make_async_copy(
                    planes.at[m, pl.ds(c * part, part)], target.at[0, 0, pl.ds(c * part, part)], left.at[m, c]
                )
            )
            leaves[-1].start()
    for leave in leaves:
        leave.wait()


def place(inner):
    return 64 * (inner // 4) + 32 * (inner // 2 % 2) + inner % 2


def swap_groups(source, target, first, last):
    lane = lax.broadcasted_iota(jnp.int32, (16, LANES), 1)
    first_half = lane < 64
    even_group = (lane & 32) == 0
    for m in range(2):
        for q in range(4):
            for g in range(4):
                v = []
                for r in range(4):
                    s = 4 * g + r
                    rows = pl.ds(place(s), 16, stride=2) if first else pl.ds(s, 16, stride=24)
                    v.append(source[m, q, rows, :])
                for r in range(2):
                    a, b = v[r], v[r + 2]
                    c = pltpu.roll(jnp.where(first_half, b, a), 64, 1)
                    v[r] = jnp.where(first_half, a, c)
                    v[r + 2] = jnp.where(first_half, c, b)
                for r in (0, 2):
                    a, b = v[r], v[r + 1]
                    v[r] = jnp.where(even_group, a, pltpu.roll(b, 32, 1))
                    v[r + 1] = jnp.where(even_group, pltpu.roll(a, 96, 1), b)
                for t in range(4):
                    s = 4 * q + t
                    rows = pl.ds(place(s), 16, stride=2) if last else pl.ds(16 * s, 16)
                    target[m, g, rows, :] = v[t]


def multiply(real, imag, tables, left, ready):
    rows = real.shape[0]
    for k, plane in enumerate((real, imag, real + imag)):
        left[k, :rows], left[k, rows:] = halves(plane)
    width = real.shape[1]
    step = 256
    for n in range(width // step):
        columns = slice(n * step, (n + 1) * step)
        terms = []
        for k in range(3):
            if n == 0:
                ready(k)
            right_h, right_l = (table[place, :, columns] for table, place in tables[2 * k:2 * k + 2])
            both = dot(left[k], right_h)
            terms.append(both[:rows] + both[rows:] + dot(left[k, :rows], right_l))
        out_real, out_imag = terms[0] - terms[1], terms[2] - terms[0] - terms[1]
        for j in range(step // LANES):
            tile = slice(j * LANES, (j + 1) * LANES)
            yield n * (step // LANES) + j, out_real[:, tile], out_imag[:, tile]


def stages_kernel(received, first, stored, sent, work, turned, later, left, arrived):
    rows = received.shape[0] // 8
    fetches = [
        pltpu.make_async_copy(stored.at[span], later.at[span], arrived.at[p]) for p, span in enumerate(spans())
    ]
    for p, fetch in enumerate(fetches):
        fetch.start(priority=min(p, 1))

    for p, span in enumerate(spans()):
        if p == 0:
            real, imag = (
                jnp.concatenate([received[pl.ds(4 * m + q, rows, stride=8), :] for q in range(4)], axis=1)
                for m in range(2)
            )
        else:
            swap_groups(work, turned, p == 1, p == PRODUCTS - 1)
            real, imag = (jnp.concatenate([turned[m, q] for q in range(4)], axis=1) for m in range(2))
        tables = [(later, span.start + j) for j in range(span.size)]
        if p == 0:
            tables = [(first, j) for j in range(4)] + tables

        def ready(k, p=p):
            if k == (2 if p == 0 else 0):
                fetches[p].wait()

        for q, out_real, out_imag in multiply(real, imag, tables, left, ready):
            if p == 0:
                work[0, q, :rows] = out_real
                work[1, q, :rows] = out_imag
            elif p < PRODUCTS - 1:
                for u in range(16):
                    work[0, q, 24 * u:24 * u + 16] = out_real[16 * u:16 * u + 16]
                    work[1, q, 24 * u:24 * u + 16] = out_imag[16 * u:16 * u + 16]
            else:
                sent[pl.ds(q, rows, stride=8), :] = out_real
                sent[pl.ds(4 + q, rows, stride=8), :] = out_imag


VMEM = pl.BlockSpec(memory_space=pltpu.VMEM)
HBM = pl.BlockSpec(memory_space=pltpu.HBM)


def call(kernel, out, ins, outs, flops, scratch=(), limit=None):
    return pl.pallas_call(
        kernel,
        out_shape=out,
        in_specs=ins,
        out_specs=outs,
        scratch_shapes=scratch,
        compiler_params=pltpu.CompilerParams(vmem_limit_bytes=limit),
        cost_estimate=pl.CostEstimate(flops=flops, bytes_accessed=2**21, transcendentals=0),
    )


def exchange(packed):
    pieces = packed.reshape(-1, 8, LANES)
    pieces = lax.all_to_all(pieces, ORDER, split_axis=0, concat_axis=0, tiled=True)
    return pieces.reshape(packed.shape)


def on_device(stem_real, stem_imag, branch_real, branch_imag, orders):
    rows, width = stem_real.shape[2:]
    packed = jax.ShapeDtypeStruct((rows * 8, LANES), jnp.float32)
    plane = jax.ShapeDtypeStruct(stem_real.shape, jnp.float32)
    planes = pltpu.VMEM((2, rows, width), jnp.float32)
    tiled = pltpu.VMEM((2, 4, rows, LANES), jnp.float32)
    dma = pltpu.SemaphoreType.DMA
    scratch = [planes, pltpu.VMEM(packed.shape, packed.dtype), dma((2, PARTS)), dma((PARTS,))]
    sent = call(pack_kernel, packed, [HBM] * 2, HBM, 10**6, scratch)(stem_real, stem_imag)
    first = jax.ShapeDtypeStruct((4, width, width), jnp.bfloat16)
    stored = jax.ShapeDtypeStruct((6 * PRODUCTS - 4, width, width), jnp.bfloat16)
    first, stored = call(
        tables_kernel, (first, stored), [VMEM] * 3, (VMEM, VMEM), 32 * width**3, (), 32 * 2**20
    )(branch_real, branch_imag, orders)
    received = exchange(sent)
    scratch = [
        pltpu.VMEM((2, 4, 384, LANES), jnp.float32),
        tiled,
        pltpu.VMEM(stored.shape, stored.dtype),
        pltpu.VMEM((3, 2 * rows, width), stored.dtype),
        dma((PRODUCTS,)),
    ]
    flops = 2 * 36 * rows * width**2
    sent = call(stages_kernel, packed, [VMEM, VMEM, HBM], VMEM, flops, scratch, 40 * 2**20)(
        received, first, stored
    )
    received = exchange(sent)
    scratch = [planes, dma((2, PARTS))]
    return tuple(
        call(unpack_kernel, (plane, plane), [VMEM], (HBM, HBM), 10**6, scratch, 4 * 2**20)(received)
    )


def solution(mesh):
    chips = Mesh(mesh.devices.reshape(4, 4, 4, 2, 2), ("zlo", "y", "x", "zhi", "core"))
    stem = P(("zlo", "y"), ("x", "zhi", "core"), None, None)
    return jax.shard_map(
        on_device,
        mesh=chips,
        in_specs=(stem, stem, P(), P(), P()),
        out_specs=(stem, stem),
        check_vma=False,
    )
```
